32 devices in a mesh: dp: 1 (over z), tp: 32 (over y, x, core).
Axes of the slice: x: 4, y: 4, z: 1, core: 2. Of those that a mesh axis runs over, the one named last changes fastest.
The devices are a block of a 4x4x8 slice.
Arguments:
- x_in: bfloat16 [2048, 8192], P(('dp', 'tp'))
- w_in: bfloat16 [8192, 28672], P(None, 'tp')
- grad_out: bfloat16 [2048, 28672], P('dp', 'tp')
Outputs:
- output 1: bfloat16 [2048, 8192], P(('dp', 'tp'))
- output 2: float32 [8192, 28672], P('dp', 'tp')
All inputs are finite; a program needn't handle non-finite values.
Results may differ from the reference program's by a relative error of at most 0.001.
Values are sent between devices in bfloat16 or wider.
A program may use at most 768 MiB of HBM per device.

```python
import jax
import jax.numpy as jnp

TOKENS = 2048
HIDDEN = 8192
FFN_DIM = 28672


def setup_inputs(seed: int = 0, part: int = 0) -> dict:
    base_key = jax.random.key(seed)
    part_key = jax.random.fold_in(base_key, part)
    key_x, key_grad = jax.random.split(part_key)
    key_weight = jax.random.key(seed + 1)
    x_in = jax.random.normal(key_x, (TOKENS, HIDDEN), jnp.float32).astype(jnp.bfloat16)
    w_in = (jax.random.normal(key_weight, (HIDDEN, FFN_DIM), jnp.float32) * HIDDEN ** -0.5).astype(jnp.bfloat16)
    grad_scale = (HIDDEN / FFN_DIM) ** 0.5
    grad_out = (jax.random.normal(key_grad, (TOKENS, FFN_DIM), jnp.float32) * grad_scale).astype(jnp.bfloat16)
    return {"x_in": x_in, "w_in": w_in, "grad_out": grad_out}


def reference(x_in, w_in, grad_out):
    grad_x = jnp.dot(grad_out, w_in.T, preferred_element_type=jnp.float32).astype(jnp.bfloat16)
    grad_w = jnp.dot(x_in.T, grad_out, preferred_element_type=jnp.float32)
    return (grad_x, grad_w)
```

```python
import jax
import jax.numpy as jnp
from jax import lax
from jax.sharding import PartitionSpec as P


OTHER = {"x": "y", "y": "x"}
WAYS = (("x", 1), ("x", -1), ("y", 1), ("y", -1))


def solution(mesh):
    n = mesh.shape["tp"]
    side = int(round((n // 2) ** 0.5))

    def device(y, x, core):
        return ((y % side) * side + x % side) * 2 + core

    def shift(axis, step):
        perm = []
        for y in range(side):
            for x in range(side):
                for core in range(2):
                    to = device(y, x + step, core) if axis == "x" else device(y + step, x, core)
                    perm.append((device(y, x, core), to))
        return perm

    swap = [(i, i ^ 1) for i in range(n)]

    def dot(a, b):
        return lax.dot_general(a, b, (((1,), (1,)), ((), ())), preferred_element_type=jnp.float32)

    def after(value, *earlier):
        return lax.optimization_barrier((value, *earlier))[0]

    def send(t, sign, along):
        return lax.ppermute(t, "tp", shift(along, sign))

    def per_device(x_blk, w_blk, grad_blk):
        me = lax.axis_index("tp")
        core = me % 2
        pos = {"x": (me // 2) % side, "y": me // (2 * side)}
        rows, hidden = x_blk.shape
        tokens, cols = grad_blk.shape
        half = hidden // 2
        chip = tokens // (side * side)
        width = half // 4

        x_full = lax.all_gather(x_blk, "tp", axis=0, tiled=True)

        g_both = jnp.concatenate([grad_blk, lax.ppermute(grad_blk, "tp", swap)], axis=1)
        w_both = []
        for q in range(4):
            give = lax.dynamic_slice_in_dim(w_blk, (1 - core) * half + q * width, width, 0)
            keep = lax.dynamic_slice_in_dim(w_blk, core * half + q * width, width, 0)
            w_both.append(jnp.concatenate([keep, lax.ppermute(give, "tp", swap)], axis=1))
        quarter = {way: w_both[q] for q, way in enumerate(WAYS)}

        def term(g, axis, ahead, way):
            g4 = g.reshape(side, side, chip, 2 * cols)
            g4 = lax.dynamic_index_in_dim(g4, (pos[axis] + ahead) % side, 1 if axis == "x" else 0, keepdims=False)
            return dot(g4.reshape(side * chip, 2 * cols), quarter[way])

        def cells(t, axis, ahead):
            return lax.dynamic_index_in_dim(t, (pos[OTHER[axis]] + ahead) % side, 0, keepdims=False)

        far, near, early, late, kept = {}, {}, {}, {}, {}
        sent = []
        for axis, sign in WAYS:
            t = term(g_both, axis, 2, (axis, sign))
            far[axis, sign] = send(t, sign, axis)
            sent.append(t)
        g_a = after(g_both, *sent)
        sent = []
        for axis, sign in WAYS:
            t = term(g_a, axis, sign, (axis, -sign))
            near[axis, sign] = send(t, sign, axis)
            sent.append(t)
        g_b = after(g_both, *sent)
        sent = []
        order = (1, -1, 0)
        for axis, sign in WAYS:
            t = (term(g_b, axis, sign, (axis, sign)) + far[axis, sign]).reshape(side, chip, width)
            early[axis, sign] = send(cells(t, axis, 2), sign, axis)
            late[axis, sign] = send(jnp.stack([cells(t, axis, k) for k in order]), sign, axis)
            sent.append(t)
        g_c = after(g_both, *sent)
        own = {way: term(g_c, way[0], 0, way) for way in WAYS}
        own = lax.optimization_barrier(own)
        for axis, sign in WAYS:
            kept[axis, sign] = own[axis, sign].reshape(side, chip, width)

        grad_w = lax.dot_general(x_full, grad_blk, (((0,), (0,)), ((), ())), preferred_element_type=jnp.float32)

        def cell(axis, sign, ahead):
            mine = cells(kept[axis, sign], axis, ahead) + cells(near[axis, -sign].reshape(side, chip, width), axis, ahead)
            return mine + (early[axis, sign] if ahead == 2 else late[axis, sign][order.index(ahead)])

        far2, near2, last2 = {}, {}, {}
        for axis, sign in WAYS:
            far2[axis, sign] = send(cell(axis, sign, 2), sign, OTHER[axis])
        for axis, sign in WAYS:
            near2[axis, sign] = send(cell(axis, -sign, sign), sign, OTHER[axis])
        for axis, sign in WAYS:
            last2[axis, sign] = send(cell(axis, sign, sign) + far2[axis, sign], sign, OTHER[axis])
        mine = jnp.concatenate(
            [cell(axis, sign, 0) + near2[axis, -sign] + last2[axis, sign] for axis, sign in WAYS], axis=1
        ).astype(jnp.bfloat16)
        keep = lax.dynamic_slice_in_dim(mine, core * rows, rows, 0)
        give = lax.dynamic_slice_in_dim(mine, (1 - core) * rows, rows, 0)
        take = lax.ppermute(give, "tp", swap)
        grad_x = jnp.where(core == 0, jnp.concatenate([keep, take], 1), jnp.concatenate([take, keep], 1))
        return grad_x, grad_w

    return jax.shard_map(
        per_device,
        mesh=mesh,
        in_specs=(P(("dp", "tp"), None), P(None, "tp"), P("dp", "tp")),
        out_specs=(P(("dp", "tp"), None), P("dp", "tp")),
        check_vma=False,
    )
```

```python
import functools

import jax
import jax.numpy as jnp
from jax import lax
from jax.experimental import pallas as pl
from jax.experimental.pallas import tpu as pltpu
from jax.sharding import PartitionSpec as P


MESH = pl.DeviceIdType.MESH
OTHER = {"x": "y", "y": "x"}
ORDER = (1, -1, 0)
WAYS = (("x", 1), ("x", -1), ("y", 1), ("y", -1))


def second_axis_kernel(side, *refs):
    own, near, early, late = (refs[4 * i : 4 * i + 4] for i in range(4))
    out_ref, parts, outbox, inbox, mine, theirs, load_sem, send_sem, recv_sem, swap_send, swap_recv, out_sem = refs[16:]
    me = lax.axis_index("tp")
    core, x, y = lax.rem(me, 2), lax.rem(me // 2, side), me // (2 * side)
    chip, width = parts.shape[3], parts.shape[4]
    rows = chip // 2

    def at(yy, xx, cc):
        return ((yy * side) + xx) * 2 + cc

    def neighbour(axis, sign):
        step = 1 if sign > 0 else side - 1
        return at(y, lax.rem(x + step, side), core) if axis == "x" else at(lax.rem(y + step, side), x, core)

    partner = at(y, x, 1 - core)
    barrier = pltpu.get_barrier_semaphore()
    for axis, sign in WAYS:
        pl.semaphore_signal(barrier, inc=1, device_id={"tp": neighbour(axis, sign)}, device_id_type=MESH)
    pl.semaphore_signal(barrier, inc=1, device_id={"tp": partner}, device_id_type=MESH)

    def loads(w, ahead):
        axis, _ = WAYS[w]
        slot = (ahead + side) % side
        b = lax.rem((y if axis == "x" else x) + slot, side)
        last = early[w] if ahead == 2 else late[w].at[ORDER.index(ahead)]
        sources = (own[w].at[b], near[w].at[b], last)
        return [
            pltpu.make_async_copy(src, parts.at[w, slot, i], load_sem.at[w, slot, i]) for i, src in enumerate(sources)
        ]

    for ahead_of in (lambda s: 2, lambda s: -s, lambda s: s, lambda s: 0):
        for w, (axis, sign) in enumerate(WAYS):
            for copy in loads(w, ahead_of(sign)):
                copy.start()

    def arrived(w, ahead):
        for copy in loads(w, ahead):
            copy.wait()
        return parts.at[w, (ahead + side) % side]

    def each(body):
        def step(i, carry):
            body(pl.ds(pl.multiple_of(i * 16, 16), 16))
            return carry

        lax.fori_loop(0, chip // 16, step, 0)

    def send(slot, w, way):
        return pltpu.make_async_remote_copy(
            src_ref=outbox.at[slot, w],
            dst_ref=inbox.at[slot, w],
            send_sem=send_sem.at[slot, w],
            recv_sem=recv_sem.at[slot, w],
            device_id={"tp": neighbour(OTHER[way[0]], way[1])},
            device_id_type=MESH,
        )

    pl.semaphore_wait(barrier, 5)
    for w, way in enumerate(WAYS):
        cell = arrived(w, 2)

        def body(r, cell=cell, w=w):
            outbox[0, w, r, :] = cell[0, r, :] + cell[1, r, :] + cell[2, r, :]

        each(body)
        send(0, w, way).start()
    for w, (axis, sign) in enumerate(WAYS):
        cell = arrived(w ^ 1, sign)

        def body(r, cell=cell, w=w):
            outbox[1, w, r, :] = cell[0, r, :] + cell[1, r, :] + cell[2, r, :]

        each(body)
        send(1, w, (axis, sign)).start()
    for w, way in enumerate(WAYS):
        cell = arrived(w, way[1])
        send(0, w, way).wait_recv()

        def body(r, cell=cell, w=w):
            outbox[2, w, r, :] = cell[0, r, :] + cell[1, r, :] + cell[2, r, :] + inbox[0, w, r, :]

        each(body)
        send(2, w, way).start()

    def swap(w):
        away = pl.ds(pl.multiple_of((1 - core) * rows, rows), rows)
        return pltpu.make_async_remote_copy(
            src_ref=mine.at[w, away],
            dst_ref=theirs.at[w],
            send_sem=swap_send.at[w],
            recv_sem=swap_recv.at[w],
            device_id={"tp": partner},
            device_id_type=MESH,
        )

    def columns(which, w):
        return pl.ds(pl.multiple_of((which * 4 + w) * width, width), width)

    def put(src, which, w, i):
        return pltpu.make_async_copy(src, out_ref.at[:, columns(which, w)], out_sem.at[w, i])

    here = pl.ds(pl.multiple_of(core * rows, rows), rows)
    for w, way in enumerate(WAYS):
        cell = arrived(w, 0)
        send(1, w ^ 1, WAYS[w ^ 1]).wait_recv()
        send(2, w, way).wait_recv()

        def body(r, cell=cell, w=w):
            total = cell[0, r, :] + cell[1, r, :] + cell[2, r, :] + inbox[1, w ^ 1, r, :] + inbox[2, w, r, :]
            mine[w, r, :] = total.astype(mine.dtype)

        each(body)
        swap(w).start()
        put(mine.at[w, here], core, w, 0).start()
    for w, way in enumerate(WAYS):
        swap(w).wait_recv()
        put(theirs.at[w], 1 - core, w, 1).start()
    for w, way in enumerate(WAYS):
        for slot in range(3):
            send(slot, w, way).wait_send()
        swap(w).wait_send()
        put(mine.at[w, here], core, w, 0).wait()
        put(theirs.at[w], 1 - core, w, 1).wait()


def second_axis(side, rows, own, near, early, late):
    _, chip, width = own[0].shape
    sent = 12 * chip * width * 4
    return pl.pallas_call(
        functools.partial(second_axis_kernel, side),
        out_shape=jax.ShapeDtypeStruct((rows, 8 * width), jnp.bfloat16),
        in_specs=[pl.BlockSpec(memory_space=pl.ANY)] * 16,
        out_specs=pl.BlockSpec(memory_space=pl.ANY),
        scratch_shapes=[
            pltpu.VMEM((4, side, 3, chip, width), jnp.float32),
            pltpu.VMEM((3, 4, chip, width), jnp.float32),
            pltpu.VMEM((3, 4, chip, width), jnp.float32),
            pltpu.VMEM((4, chip, width), jnp.bfloat16),
            pltpu.VMEM((4, rows, width), jnp.bfloat16),
            pltpu.SemaphoreType.DMA((4, side, 3)),
            pltpu.SemaphoreType.DMA((3, 4)),
            pltpu.SemaphoreType.DMA((3, 4)),
            pltpu.SemaphoreType.DMA((4,)),
            pltpu.SemaphoreType.DMA((4,)),
            pltpu.SemaphoreType.DMA((4, 2)),
        ],
        compiler_params=pltpu.CompilerParams(
            collective_id=0, has_side_effects=True, vmem_limit_bytes=48 * 1024 * 1024
        ),
        cost_estimate=pl.CostEstimate(flops=20_000_000_000, bytes_accessed=2 * sent, transcendentals=0),
    )(*own, *near, *early, *late)


EVENTS = (0, 8, 16, 22, 34, 44, 58)


def gather_kernel(side, x_ref, w_ref, g_ref, x_full, *refs):
    terms = refs[:16]
    x_own, g_both, w_both, lhs, stage, ring_send, ring_recv, pass_send, pass_recv, swap_send, swap_recv, load_sem, stage_sem = refs[16:]
    me = lax.axis_index("tp")
    core, x, y = lax.rem(me, 2), lax.rem(me // 2, side), me // (2 * side)
    rows, hidden = x_ref.shape
    chip, cols = g_ref.shape[2], g_ref.shape[3]
    half, width, tile = hidden // 2, hidden // 8, stage.shape[3]
    part = 2 * width
    per_term = width // tile

    def at(yy, xx, cc):
        return ((yy * side) + xx) * 2 + cc

    def move(v, step):
        return lax.rem(v + (step + side) % side, side)

    def neighbour(axis, sign):
        return at(y, move(x, sign), core) if axis == "x" else at(move(y, sign), x, core)

    partner = at(y, x, 1 - core)
    barrier = pltpu.get_barrier_semaphore()
    for axis, sign in WAYS:
        pl.semaphore_signal(barrier, inc=1, device_id={"tp": neighbour(axis, sign)}, device_id_type=MESH)
    pl.semaphore_signal(barrier, inc=1, device_id={"tp": partner}, device_id_type=MESH)

    load_x = pltpu.make_async_copy(x_ref, x_own, load_sem.at[0])
    load_g = pltpu.make_async_copy(g_ref, g_both.at[:, :, :, pl.ds(0, cols)], load_sem.at[1])
    load_w = pltpu.make_async_copy(
        w_ref.at[pl.ds(pl.multiple_of(core * half, half), half)], w_both.at[:, pl.ds(0, cols)], load_sem.at[2]
    )
    for copy in (load_x, load_g, load_w):
        copy.start()
    pl.semaphore_wait(barrier, 5)

    def to_partner(src, dst, i):
        return pltpu.make_async_remote_copy(
            src_ref=src, dst_ref=dst, send_sem=swap_send.at[i], recv_sem=swap_recv.at[i],
            device_id={"tp": partner}, device_id_type=MESH,
        )

    load_x.wait()
    my_rows = x_full.at[y, x, pl.ds(pl.multiple_of(core * rows, rows), rows)]
    swap_x = to_partner(x_own, my_rows, 0)
    swap_x.start()
    put_x = pltpu.make_async_copy(x_own, my_rows, load_sem.at[3])
    put_x.start()
    swap_g = to_partner(g_ref, g_both.at[:, :, :, pl.ds(cols, cols)], 1)
    swap_w = to_partner(
        w_ref.at[pl.ds(pl.multiple_of((1 - core) * half, half), half)], w_both.at[:, pl.ds(cols, cols)], 2
    )
    put_x.wait()
    swap_x.wait_recv()

    def cell(p, du, dv, which):
        yy, xx = (move(y, du), move(x, dv)) if p == 0 else (move(y, dv), move(x, du))
        lo = core * half + p * part + (width if which == "B" else 0)
        size = part if which == "all" else width
        return x_full.at[yy, xx, :, pl.ds(pl.multiple_of(lo, width), size)]

    def ring(p, kind, s, du, dv, which):
        first = kind < 2
        axis = ("y" if first else "x") if p == 0 else ("x" if first else "y")
        block = cell(p, du, dv, which)
        return pltpu.make_async_remote_copy(
            src_ref=block, dst_ref=block, send_sem=ring_send.at[p, kind, s], recv_sem=ring_recv.at[p, kind, s],
            device_id={"tp": neighbour(axis, 1 - 2 * s)}, device_id_type=MESH,
        )

    def hand(p, du, dv):
        block, i = cell(p, du, dv, "all"), (du % side) * side + dv % side
        return pltpu.make_async_remote_copy(
            src_ref=block, dst_ref=block, send_sem=pass_send.at[p, i], recv_sem=pass_recv.at[p, i],
            device_id={"tp": partner}, device_id_type=MESH,
        )

    offsets = (0, 1, -1, 2)
    both = [(p, s) for p in range(2) for s in range(2)]

    def u1(p, s):
        return ring(p, 0, s, 0, 0, "all")

    def u2(p, s):
        return ring(p, 1, s, 2 * s - 1, 0, "AB"[s])

    def v1(p, s, k):
        return ring(p, 2 + k, s, offsets[k], 0, "all")

    def v2(p, s, k):
        return ring(p, 6 + k, s, offsets[k], 2 * s - 1, "AB"[s])

    def event0():
        for p, s in both:
            u1(p, s).start()
        for p, s in both:
            v1(p, s, 0).start()
        swap_g.start()
        swap_w.start()
        load_g.wait()
        load_w.wait()
        swap_g.wait_recv()
        swap_w.wait_recv()

    def event1():
        for p, s in both:
            u1(p, s).wait_recv()
        for p, s in both:
            u2(p, s).start()
        for k in (1, 2):
            for p, s in both:
                v1(p, s, k).start()
        for p in range(2):
            hand(p, 1, 0).start()
            hand(p, -1, 0).start()

    def second(k):
        for p, s in both:
            v1(p, s, k).wait_recv()
        for p, s in both:
            v2(p, s, k).start()
        for p in range(2):
            hand(p, offsets[k], 1).start()
            hand(p, offsets[k], -1).start()

    def third(k):
        for p, s in both:
            v2(p, s, k).wait_recv()
        for p in range(2):
            hand(p, offsets[k], 2).start()

    def event2():
        second(0)

    def event3():
        for p, s in both:
            u2(p, s).wait_recv()
        for p, s in both:
            v1(p, s, 3).start()
        for p in range(2):
            hand(p, 2, 0).start()

    def event4():
        second(1)
        third(0)

    def event5():
        second(2)

    def event6():
        second(3)
        third(1)
        third(2)

    events = (event0, event1, event2, event3, event4, event5, event6)

    def stored(slot):
        return pltpu.make_async_copy(stage.at[slot], terms[0].at[:, :, pl.ds(0, tile)], stage_sem.at[slot])

    def step(t, carry):
        for when, event in zip(EVENTS, events):
            pl.when(t == when)(event)
        o, j, slot = t // per_term, lax.rem(t, per_term), lax.rem(t, 2)
        kind, w = o // 4, lax.rem(o, 4)
        ax, sign = w // 2, 1 - 2 * lax.rem(w, 2)
        middle = lax.rem((kind + 1) // 2, 2)
        ahead = 2 * (1 - (kind + 3) // 4) + middle * sign
        q = w + middle * (2 - kind) * sign
        b = lax.rem((1 - ax) * x + ax * y + ahead + side, side)

        @pl.when(j == 0)
        def _():
            for i in range(side):
                lhs[i * chip : (i + 1) * chip, :] = g_both[(1 - ax) * i + ax * b, (1 - ax) * b + ax * i]

        @pl.when(t >= 2)
        def _():
            stored(slot).wait()

        rhs = w_both[pl.ds(pl.multiple_of(q * width + j * tile, tile), tile), :]
        term = lax.dot_general(lhs[...], rhs, (((1,), (1,)), ((), ())), preferred_element_type=jnp.float32)
        stage[slot] = term.reshape(side, chip, tile)
        for i in range(16):

            @pl.when(o == i)
            def _():
                to = terms[i].at[:, :, pl.ds(pl.multiple_of(j * tile, tile), tile)]
                pltpu.make_async_copy(stage.at[slot], to, stage_sem.at[slot]).start()

        return carry

    lax.fori_loop(0, 16 * per_term, step, 0)
    stored(0).wait()
    stored(1).wait()
    third(3)
    for p, s in both:
        u1(p, s).wait_send()
        u2(p, s).wait_send()
        for k in range(4):
            v1(p, s, k).wait_send()
            v2(p, s, k).wait_send()
    for copy in (swap_x, swap_g, swap_w):
        copy.wait_send()
    for p in range(2):
        for du in offsets:
            for dv in offsets:
                if du or dv:
                    hand(p, du, dv).wait()


def gather(side, x_blk, w_blk, g4):
    rows, hidden = x_blk.shape
    chip, cols = g4.shape[2:]
    width = hidden // 8
    tile = 256
    term = jax.ShapeDtypeStruct((side, chip, width), jnp.float32)
    sent = 2 * side * side * chip * hidden
    return pl.pallas_call(
        functools.partial(gather_kernel, side),
        out_shape=[jax.ShapeDtypeStruct((side, side, chip, hidden), x_blk.dtype)] + [term] * 16,
        in_specs=[pl.BlockSpec(memory_space=pl.ANY)] * 3,
        out_specs=[pl.BlockSpec(memory_space=pl.ANY)] * 17,
        scratch_shapes=[
            pltpu.VMEM((rows, hidden), x_blk.dtype),
            pltpu.VMEM((side, side, chip, 2 * cols), g4.dtype),
            pltpu.VMEM((hidden // 2, 2 * cols), w_blk.dtype),
            pltpu.VMEM((side * chip, 2 * cols), g4.dtype),
            pltpu.VMEM((2, side, chip, tile), jnp.float32),
            pltpu.SemaphoreType.DMA((2, 10, 2)),
            pltpu.SemaphoreType.DMA((2, 10, 2)),
            pltpu.SemaphoreType.DMA((2, side * side)),
            pltpu.SemaphoreType.DMA((2, side * side)),
            pltpu.SemaphoreType.DMA((3,)),
            pltpu.SemaphoreType.DMA((3,)),
            pltpu.SemaphoreType.DMA((4,)),
            pltpu.SemaphoreType.DMA((2,)),
        ],
        compiler_params=pltpu.CompilerParams(
            collective_id=1, has_side_effects=True, vmem_limit_bytes=56 * 1024 * 1024
        ),
        cost_estimate=pl.CostEstimate(flops=60_000_000_000, bytes_accessed=2 * sent, transcendentals=0),
    )(x_blk, w_blk, g4)


def solution(mesh):
    n = mesh.shape["tp"]
    side = int(round((n // 2) ** 0.5))

    def device(y, x, core):
        return ((y % side) * side + x % side) * 2 + core

    def shift(axis, step):
        perm = []
        for y in range(side):
            for x in range(side):
                for core in range(2):
                    to = device(y, x + step, core) if axis == "x" else device(y + step, x, core)
                    perm.append((device(y, x, core), to))
        return perm

    def send(t, sign, along):
        return lax.ppermute(t, "tp", shift(along, sign))

    def per_device(x_blk, w_blk, grad_blk):
        me = lax.axis_index("tp")
        pos = {"x": (me // 2) % side, "y": me // (2 * side)}
        rows, hidden = x_blk.shape
        tokens, cols = grad_blk.shape
        chip = tokens // (side * side)

        x_full, *terms = gather(side, x_blk, w_blk, grad_blk.reshape(side, side, chip, cols))
        x_full = x_full.reshape(tokens, hidden)
        terms = {(kind, way): terms[4 * kind + w] for kind in range(4) for w, way in enumerate(WAYS)}

        def cells(t, axis, ahead):
            return lax.dynamic_index_in_dim(t, (pos[OTHER[axis]] + ahead) % side, 0, keepdims=False)

        far, near, early, late = {}, {}, {}, {}
        for axis, sign in WAYS:
            far[axis, sign] = send(terms[0, (axis, sign)], sign, axis)
        for axis, sign in WAYS:
            near[axis, sign] = send(terms[1, (axis, sign)], sign, axis)
        for axis, sign in WAYS:
            t = terms[2, (axis, sign)] + far[axis, sign]
            early[axis, sign] = send(cells(t, axis, 2), sign, axis)
            late[axis, sign] = send(jnp.stack([cells(t, axis, k) for k in ORDER]), sign, axis)

        grad_w = lax.dot_general(x_full, grad_blk, (((0,), (0,)), ((), ())), preferred_element_type=jnp.float32)

        grad_x = second_axis(
            side,
            rows,
            [terms[3, way] for way in WAYS],
            [near[axis, -sign] for axis, sign in WAYS],
            [early[way] for way in WAYS],
            [late[way] for way in WAYS],
        )
        return grad_x, grad_w

    return jax.shard_map(
        per_device,
        mesh=mesh,
        in_specs=(P(("dp", "tp"), None), P(None, "tp"), P("dp", "tp")),
        out_specs=(P(("dp", "tp"), None), P("dp", "tp")),
        check_vma=False,
    )
```
